32 devices in a mesh: seq: 8 (over z, x), head: 4 (over y, core).
Axes of the slice: x: 2, y: 2, z: 4, core: 2. Of those that a mesh axis runs over, the one named last changes fastest.
Arguments:
- queries: bfloat16 [4096, 4096], P('seq', 'head'), may hold values from -120 to 120
- keys: bfloat16 [4096, 1024], P('seq', 'head'), may hold values from -4 to 4
- values: bfloat16 [4096, 1024], P('seq', 'head'), may hold values from -6 to 6
- doc_start: int32 [4096], P('seq'), may hold values from 0 to 4095, as said below
- hop_counts: int32 [8], P('seq'), may hold values from 0 to 4, as said below
- loss_mask: int32 [4096], P('seq'), may hold values from 0 to 1, as said below
Outputs:
- attention: bfloat16 [4096, 4096], P('seq', 'head')
- objective: float32 [], replicated
The draws below stay inside these ranges and needn't reach their ends.
Inputs may be any that keep to these rules, and one draw needn't show every extreme that they name: doc_start is nondecreasing; doc_start[doc_start[i]] = doc_start[i] <= i; a document holds at most 2048 tokens, and some document holds exactly that many in every draw. hop_counts[b] = b - floor(doc_start[b * 512] / 512); the most, 4, is reached in every draw. loss_mask[0] = 1.
All inputs are finite; a program needn't handle non-finite values.
Results may differ from the reference program's by a relative error of at most 0.0035.
Values may be sent and summed in bfloat16 or wider, within the bound.
A program may use at most 128 MiB of HBM per device.

```python
import math
import jax
import jax.numpy as jnp
from jax import lax

QUERY_HEADS = 32
KEY_VALUE_HEADS = 8
HEAD_WIDTH = 128
BLOCK_TOKENS = 512
HOPS = 4
PACKED_TOKENS = 4096


def doc_layout(key):
    span = HOPS * BLOCK_TOKENS
    places = jnp.arange(PACKED_TOKENS, dtype=jnp.int32)
    windows = PACKED_TOKENS // span + 2
    rates = jax.random.randint(jax.random.fold_in(key, 11), (windows,), 0, 3)
    levels = jnp.array([2, 4, 8], dtype=jnp.int32)[rates]
    whole_window = jax.random.randint(jax.random.fold_in(key, 13), (), 0, max(PACKED_TOKENS // span - 1, 1))
    window_ids = jnp.arange(windows, dtype=jnp.int32)
    levels = jnp.where(window_ids == whole_window, 0, levels)
    ticket = jax.random.randint(jax.random.fold_in(key, 12), (PACKED_TOKENS,), 0, span)
    window_of = jnp.maximum(places - 1, 0) // span
    flagged = (places % span == 1) | (places == 0) | (places == PACKED_TOKENS - 1) | (ticket < levels[window_of])
    starts = lax.cummax(jnp.where(flagged, places, 0), axis=0)
    block_ids = jnp.arange(PACKED_TOKENS // BLOCK_TOKENS, dtype=jnp.int32)
    hops = block_ids - starts[block_ids * BLOCK_TOKENS] // BLOCK_TOKENS
    return (starts.astype(jnp.int32), hops.astype(jnp.int32))


def draw_doc_start(key, part):
    return doc_layout(key)[0]


def draw_hop_counts(key, part):
    return doc_layout(key)[1]


def draw_loss_mask(key, part):
    places = jnp.arange(PACKED_TOKENS, dtype=jnp.int32)
    ticket = jax.random.randint(jax.random.fold_in(key, 31), (PACKED_TOKENS,), 0, 1000)
    marks = (ticket < 200 + 500 * places // PACKED_TOKENS).astype(jnp.int32)
    return marks.at[0].set(1)


def query_keys(key):
    resident_keys = jnp.clip(jax.random.normal(jax.random.fold_in(key, 21), (PACKED_TOKENS, KEY_VALUE_HEADS * HEAD_WIDTH), jnp.float32), -4.0, 4.0)
    base_queries = jnp.clip(jax.random.normal(jax.random.fold_in(key, 22), (PACKED_TOKENS, QUERY_HEADS * HEAD_WIDTH), jnp.float32), -4.0, 4.0)
    return (base_queries, resident_keys)


def draw_queries(key, part):
    return query_keys(key)[0].astype(jnp.bfloat16)


def draw_keys(key, part):
    return query_keys(key)[1].astype(jnp.bfloat16)


def block_levels(rng, shape, pieces, low, top_value):
    level = 1.0
    for dim, shards_of in pieces:
        steps = jax.random.uniform(jax.random.fold_in(jax.random.fold_in(rng, 6), dim), (shards_of,), jnp.float32, low / len(pieces), top_value / len(pieces))
        level = level * jnp.repeat(jnp.exp(steps), shape[dim] // shards_of).reshape((-1,) + (1,) * (len(shape) - 1 - dim))
    return level


def centred(stream_key, extent, scale, reach, pieces=(), kind=jnp.bfloat16):
    level = block_levels(stream_key, extent, pieces, -0.22, 0.18) if pieces else 1.0
    result = jax.random.normal(stream_key, extent, jnp.float32) * scale * level
    return jnp.minimum(jnp.maximum(result, -reach), reach).astype(kind)


def setup_inputs(seed: int = 0) -> dict:
    arg_keys = jax.random.split(jax.random.key(seed), 7)
    queries = draw_queries(jax.random.fold_in(arg_keys[6], 71), 0)
    keys = draw_keys(jax.random.fold_in(arg_keys[6], 71), 0)
    values = centred(arg_keys[2], (PACKED_TOKENS, KEY_VALUE_HEADS * HEAD_WIDTH), 1.0, 6.0, ((0, 8), (1, 4)))
    doc_start = draw_doc_start(jax.random.fold_in(arg_keys[6], 71), 0)
    hop_counts = draw_hop_counts(jax.random.fold_in(arg_keys[6], 71), 0)
    loss_mask = draw_loss_mask(jax.random.fold_in(arg_keys[6], 71), 0)
    return {"queries": queries, "keys": keys, "values": values, "doc_start": doc_start, "hop_counts": hop_counts, "loss_mask": loss_mask}


def reference(queries, keys, values, doc_start, hop_counts, loss_mask):
    group_size = QUERY_HEADS // KEY_VALUE_HEADS
    blocks = PACKED_TOKENS // BLOCK_TOKENS
    border_width = HOPS * BLOCK_TOKENS
    reach_extent = (HOPS + 1) * BLOCK_TOKENS
    key_padding = jnp.concatenate([jnp.zeros((border_width, KEY_VALUE_HEADS * HEAD_WIDTH), keys.dtype), keys], axis=0)
    value_padding = jnp.concatenate([jnp.zeros((border_width, KEY_VALUE_HEADS * HEAD_WIDTH), values.dtype), values], axis=0)

    def one_block(block):
        block_offset = (block * BLOCK_TOKENS).astype(jnp.int32)
        query_row_block = lax.dynamic_slice_in_dim(queries, block_offset, BLOCK_TOKENS, 0).reshape(BLOCK_TOKENS, KEY_VALUE_HEADS, group_size, HEAD_WIDTH).astype(jnp.float32)
        key_row_block = lax.dynamic_slice_in_dim(key_padding, block_offset, reach_extent, 0).reshape(reach_extent, KEY_VALUE_HEADS, HEAD_WIDTH).astype(jnp.float32)
        value_row_block = lax.dynamic_slice_in_dim(value_padding, block_offset, reach_extent, 0).reshape(reach_extent, KEY_VALUE_HEADS, HEAD_WIDTH).astype(jnp.float32)
        scores = jnp.einsum('tgqd,sgd->tgqs', query_row_block, key_row_block) / math.sqrt(HEAD_WIDTH)
        key_place = block_offset - border_width + jnp.arange(reach_extent, dtype=jnp.int32)
        query_place = block_offset + jnp.arange(BLOCK_TOKENS, dtype=jnp.int32)
        firsts = lax.dynamic_slice_in_dim(doc_start, block_offset, BLOCK_TOKENS, 0)
        hop_limit = lax.dynamic_index_in_dim(hop_counts, block, 0, keepdims=False)
        distance = block - jnp.floor_divide(key_place, BLOCK_TOKENS)
        seen = (key_place[None, :] >= firsts[:, None]) & (key_place[None, :] <= query_place[:, None]) & (distance <= hop_limit)[None, :]
        seen = seen[:, None, None, :]
        masked = jnp.where(seen, scores, jnp.float32(-1e+30))
        top = lax.optimization_barrier(jnp.max(masked, axis=-1, keepdims=True))
        weights = jnp.where(seen, jnp.exp(masked - top), jnp.float32(0.0))
        total = lax.optimization_barrier(jnp.sum(weights, axis=-1))
        rounded = lax.optimization_barrier(weights.astype(jnp.bfloat16))
        numer = jnp.einsum('tgqs,sgd->tgqd', rounded.astype(jnp.float32), value_row_block)
        attended = (numer / total[..., None]).reshape(BLOCK_TOKENS, QUERY_HEADS * HEAD_WIDTH)
        marks = lax.dynamic_slice_in_dim(loss_mask, block_offset, BLOCK_TOKENS, 0).astype(jnp.float32)
        squares = jnp.sum(marks[:, None] * attended * attended)
        return (attended.astype(jnp.bfloat16), squares)
    outputs, squares = lax.map(one_block, jnp.arange(blocks, dtype=jnp.int32))
    attention = outputs.reshape(PACKED_TOKENS, QUERY_HEADS * HEAD_WIDTH)
    counted = jnp.sum(loss_mask.astype(jnp.float32))
    objective = jnp.sum(squares) / (QUERY_HEADS * counted)
    return (attention, objective)
```

```python
import functools
import math

import jax
import jax.numpy as jnp
from jax import lax
from jax.experimental import pallas as pl
from jax.experimental.pallas import tpu as pltpu
from jax.sharding import PartitionSpec as P

QUERY_HEADS = 32
KEY_VALUE_HEADS = 8
HEAD_WIDTH = 128
HOPS = 4

MESH = pl.DeviceIdType.MESH
CHUNK = 64
STEP = 256
DOCUMENT = 2048
LOW = -1e30

Z1, Z2, X1, X2 = range(4)
DISTANCE = {Z1: 2, Z2: 4, X1: 1, X2: 3}


def kernel(
    blocks, groups, q_ref, k_ref, v_ref, start_ref, hop_ref, mask_ref, out_ref, obj_ref,
    got_k, got_v, acc, top, first, marks, bias, joined, stat, stat_got, row, row_got,
    send_z, send_x, recv, send_s, recv_s, send_r, recv_r,
):
    rows = q_ref.shape[0]
    heads = q_ref.shape[1] // HEAD_WIDTH
    group_size = QUERY_HEADS // KEY_VALUE_HEADS
    chunks = rows // CHUNK
    per_step = STEP // CHUNK
    scale = math.log2(math.e) / math.sqrt(HEAD_WIDTH)
    b = lax.axis_index("seq")
    hd = lax.axis_index("head")
    odd = lax.rem(b, 2)
    partner = b + 1 - 2 * odd

    barrier = pltpu.get_barrier_semaphore()
    for k in range(1, groups):
        pl.semaphore_signal(
            barrier, inc=1, device_id=(b, lax.rem(hd + k, groups)), device_id_type=MESH
        )

    def greet(k, carry):
        pl.semaphore_signal(
            barrier, inc=1, device_id=(lax.rem(b + k, blocks), hd), device_id_type=MESH
        )
        return carry

    lax.fori_loop(1, blocks, greet, 0)
    pl.semaphore_wait(barrier, blocks + groups - 2)

    def pair(src_k, src_v, slot, c, send, to):
        at = pl.ds(c * CHUNK, CHUNK)
        made = []
        for which, (src, dst) in enumerate(((src_k, got_k), (src_v, got_v))):
            made.append(
                pltpu.make_async_remote_copy(
                    src_ref=src.at[at, :],
                    dst_ref=dst.at[slot, at, :],
                    send_sem=send.at[which],
                    recv_sem=recv.at[slot, c, which],
                    device_id=(to, hd),
                    device_id_type=MESH,
                )
            )
        return made

    up = b + 2
    has_up = up < blocks

    def own_z(c):
        return pair(k_ref, v_ref, Z1, c, send_z.at[0, c], up)

    def on_z(c):
        return pair(got_k.at[Z1], got_v.at[Z1], Z2, c, send_z.at[1, c], up)

    def even_first(c):
        return pair(k_ref, v_ref, X1, c, send_x.at[0, c], partner)

    def even_second(c):
        return pair(got_k.at[Z1], got_v.at[Z1], X2, c, send_x.at[1, c], partner)

    def odd_first(c):
        return pair(got_k.at[Z1], got_v.at[Z1], X1, c, send_x.at[0, c], partner)

    def odd_second(c):
        return pair(got_k.at[Z2], got_v.at[Z2], X2, c, send_x.at[1, c], partner)

    def begin(copies):
        for copy in copies:
            copy.start()

    def sent(copies):
        for copy in copies:
            copy.wait_send()

    def landed(slot, c):
        for copy in pair(k_ref, v_ref, slot, c, send_z.at[0, c], partner):
            copy.wait_recv()

    for c in range(chunks):
        @pl.when(has_up)
        def _():
            begin(own_z(c))

        @pl.when(odd == 0)
        def _():
            begin(even_first(c))

    def column(line):
        return jnp.broadcast_to(line.astype(jnp.float32), (HEAD_WIDTH, rows)).T

    first[...] = column(jnp.maximum(start_ref[...], (b - hop_ref[0]) * rows))
    marks[...] = column(mask_ref[...])
    joined[...] = jnp.ones_like(joined)

    def attend(keys, values, offset, distance, fresh=False):
        base = (b - distance) * rows + offset
        at = pl.ds(offset, STEP)
        lo = offset if distance == 0 else 0
        hi = max(0, min(rows, DOCUMENT + offset + STEP - 1 - distance * rows))
        lo, hi = lo // 128 * 128, min(rows, -(-hi // 128) * 128)
        span = slice(lo, hi)
        tile = (hi - lo, 128)
        for j in range(0, STEP, 128):
            spot = base + j + lax.broadcasted_iota(jnp.int32, tile, 1)
            seen = spot.astype(jnp.float32) >= first[span]
            if distance == 0:
                seen = seen & (spot <= b * rows + lo + lax.broadcasted_iota(jnp.int32, tile, 0))
            bias[span, j : j + 128] = jnp.where(seen, 0.0, LOW)
        for g in range(heads // group_size):
            joined[g, :, :HEAD_WIDTH] = values[at, g * HEAD_WIDTH : (g + 1) * HEAD_WIDTH]

        def one(h, g):
            lanes = pl.ds(pl.multiple_of(h * HEAD_WIDTH, HEAD_WIDTH), HEAD_WIDTH)
            kv = pl.ds(g * HEAD_WIDTH, HEAD_WIDTH)
            s = lax.dot_general(
                q_ref[span, lanes], keys[at, kv], (((1,), (1,)), ((), ())),
                preferred_element_type=jnp.float32,
            ) + bias[span]
            new = jnp.broadcast_to(jnp.max(s, axis=1, keepdims=True), tile)
            if not fresh:
                old = top[h, span]
                new = jnp.maximum(old, new)
            p = jnp.concatenate(
                [
                    jnp.exp2((s[:, j : j + 128] - new) * scale).astype(jnp.bfloat16)
                    for j in range(0, STEP, 128)
                ],
                axis=1,
            )
            update = jnp.dot(p, joined[g], preferred_element_type=jnp.float32)
            top[h, span] = new
            if not fresh:
                ratio = jnp.exp2((old - new) * scale)
                update = acc[h, span] * jnp.concatenate([ratio, ratio], axis=1) + update
            acc[h, span] = update

        def body(i, carry):
            for g in range(heads // group_size):
                one(g * group_size + i, g)
            return carry

        lax.fori_loop(0, group_size, body, 0)

    def take(slot, c):
        @pl.when(b >= DISTANCE[slot])
        def _():
            landed(slot, c)
            if slot == Z1:
                @pl.when(has_up)
                def _():
                    begin(on_z(c))

                @pl.when(odd == 0)
                def _():
                    begin(even_second(c))

                @pl.when(odd == 1)
                def _():
                    begin(odd_first(c))
            if slot == Z2:
                @pl.when(odd == 1)
                def _():
                    begin(odd_second(c))

    def work(slot, step):
        @pl.when(b >= DISTANCE[slot])
        def _():
            attend(got_k.at[slot], got_v.at[slot], step * STEP, DISTANCE[slot])

    steps = rows // STEP
    for step in range(steps):
        attend(k_ref, v_ref, step * STEP, 0, fresh=step == 0)

    for step in range(steps):
        for c in range(step * per_step, (step + 1) * per_step):
            take(Z1, c)
        work(Z1, step)
    pending = []
    for step in range(steps):
        pending.append((X1, step))
    for c in range(chunks):
        take(Z2, c)
        if c % per_step == per_step // 2 - 1 and pending:
            slot, step = pending.pop(0)
            for d in range(step * per_step, (step + 1) * per_step):
                take(slot, d)
            work(slot, step)
        if c % per_step == per_step - 1:
            step = c // per_step
            if step < steps - 1:
                work(Z2, step)
                for d in range(step * per_step, (step + 1) * per_step):
                    take(X2, d)
                work(X2, step)
            else:
                work(Z2, step)
    for slot, step in pending:
        for d in range(step * per_step, (step + 1) * per_step):
            take(slot, d)
        work(slot, step)
    last = steps - 1
    for d in range(last * per_step, (last + 1) * per_step):
        take(X2, d)
    work(X2, last)

    def finish(h):
        attended = acc[h, :, :HEAD_WIDTH] * (1.0 / acc[h, :, HEAD_WIDTH:])
        out_ref[:, h * HEAD_WIDTH : (h + 1) * HEAD_WIDTH] = attended.astype(jnp.bfloat16)
        return jnp.sum((attended * attended * marks[...]).reshape(rows // 8, 8, 128), axis=0)

    squares = finish(0)
    for h in range(1, heads):
        squares = squares + finish(h)
    stat[:8] = squares
    stat[8:] = jnp.sum(marks[...].reshape(rows // 8, 8, 128), axis=0)

    def to_head(k):
        return pltpu.make_async_remote_copy(
            src_ref=stat, dst_ref=stat_got.at[k], send_sem=send_s.at[k], recv_sem=recv_s.at[k],
            device_id=(b, lax.rem(hd + k, groups)), device_id_type=MESH,
        )

    def to_block(k):
        return pltpu.make_async_remote_copy(
            src_ref=row, dst_ref=row_got.at[k], send_sem=send_r.at[k], recv_sem=recv_r.at[k],
            device_id=(lax.rem(b + k, blocks), hd), device_id_type=MESH,
        )

    for c in range(chunks):
        @pl.when(has_up)
        def _():
            sent(own_z(c))

            @pl.when(b >= DISTANCE[Z1])
            def _():
                sent(on_z(c))

        @pl.when(odd == 0)
        def _():
            sent(even_first(c))

            @pl.when(b >= DISTANCE[Z1])
            def _():
                sent(even_second(c))

        @pl.when((odd == 1) & (b >= DISTANCE[Z1]))
        def _():
            sent(odd_first(c))

        @pl.when((odd == 1) & (b >= DISTANCE[Z2]))
        def _():
            sent(odd_second(c))
    for k in range(1, groups):
        to_head(k).start()
    whole = stat[...]
    for k in range(1, groups):
        to_head(k).wait_recv()
        whole = whole + stat_got[k]
    row[...] = whole
    for k in range(1, groups):
        to_head(k).wait_send()

    def give(k, carry):
        to_block(k).start()
        return carry

    lax.fori_loop(1, blocks, give, 0)


    def gather(k, so_far):
        to_block(k).wait()
        return so_far + row_got[k]

    final = lax.fori_loop(1, blocks, gather, row[...])
    square_sum = jnp.sum(final[:8], keepdims=True)
    count = jnp.sum(final[8:], keepdims=True) * (1.0 / (groups * 128))
    obj_ref[...] = jnp.broadcast_to(square_sum / (QUERY_HEADS * count), obj_ref.shape)


def solution(mesh):
    blocks, groups = mesh.shape["seq"], mesh.shape["head"]

    def on_device(queries, keys, values, doc_start, hop_counts, loss_mask):
        rows, width = queries.shape
        heads = width // HEAD_WIDTH
        chunks = rows // CHUNK
        vmem = pl.BlockSpec(memory_space=pltpu.VMEM)
        dma = pltpu.SemaphoreType.DMA
        attention, objective = pl.pallas_call(
            functools.partial(kernel, blocks, groups),
            out_shape=(
                jax.ShapeDtypeStruct((rows, width), jnp.bfloat16),
                jax.ShapeDtypeStruct((1, 128), jnp.float32),
            ),
            in_specs=[vmem] * 4 + [pl.BlockSpec(memory_space=pltpu.SMEM), vmem],
            out_specs=(vmem, vmem),
            scratch_shapes=[
                pltpu.VMEM((4, *keys.shape), jnp.bfloat16),
                pltpu.VMEM((4, *values.shape), jnp.bfloat16),
                pltpu.VMEM((heads, rows, 2 * HEAD_WIDTH), jnp.float32),
                pltpu.VMEM((heads, rows, 128), jnp.float32),
                pltpu.VMEM((rows, 128), jnp.float32),
                pltpu.VMEM((rows, 128), jnp.float32),
                pltpu.VMEM((rows, STEP), jnp.float32),
                pltpu.VMEM((keys.shape[1] // HEAD_WIDTH, STEP, 2 * HEAD_WIDTH), jnp.bfloat16),
                pltpu.VMEM((16, 128), jnp.float32),
                pltpu.VMEM((groups, 16, 128), jnp.float32),
                pltpu.VMEM((16, 128), jnp.float32),
                pltpu.VMEM((blocks, 16, 128), jnp.float32),
                dma((2, chunks, 2)),
                dma((2, chunks, 2)),
                dma((4, chunks, 2)),
                dma((groups,)),
                dma((groups,)),
                dma((blocks,)),
                dma((blocks,)),
            ],
            compiler_params=pltpu.CompilerParams(collective_id=0, has_side_effects=True),
        )(
            queries, keys, values, doc_start.reshape(1, rows), hop_counts,
            loss_mask.reshape(1, rows),
        )
        return attention, objective[0, 0]

    placed = (P("seq", "head"), P("seq", "head"), P("seq", "head"), P("seq"), P("seq"), P("seq"))
    return jax.shard_map(
        on_device, mesh=mesh, in_specs=placed, out_specs=(P("seq", "head"), P()), check_vma=False
    )
```
